256 devices in a mesh: ao: 32 (over x_lo, z, core), gen: 4 (over y), act: 2 (over x_hi).
Axes of the slice: x: 4 (x_hi: 2, x_lo: 2; x = x_hi * 2 + x_lo), y: 4, z: 8, core: 2. Of those that a mesh axis runs over, the one named last changes fastest.
Arguments:
- integrals: bfloat16 [3072, 2, 128, 1152], P(('ao', 'gen', 'act')), may hold values from -24 to 24
- bra_rows: bfloat16 [3072, 2, 128, 16], P(('ao', 'gen', 'act')), may hold values from -0.009765625 to 0.009765625
- ket_rows: bfloat16 [3072, 2, 128, 48], P(('ao', 'gen', 'act')), may hold values from -6 to 6
- block_count: int32 [256], P(('ao', 'gen', 'act')), may hold values from 1 to 12, as said below
- pair_count: int32 [3072], P(('ao', 'gen', 'act')), may hold values from 32 to 128
Outputs:
- transformed: float32 [2, 16, 48, 1152], P(None, 'gen', 'act', 'ao')
The draws below stay inside these ranges and needn't reach their ends.
Inputs may be any that keep to these rules, and one draw needn't show every extreme that they name: `block_count`: one device holds exactly 12 live blocks. Rows from pair_count on are padding.
All inputs are finite; a program needn't handle non-finite values.
Results may differ from the reference program's by a relative error of at most 0.0042.
Values may be sent and summed in bfloat16 or wider, within the bound.
A program may use at most 128 MiB of HBM per device.

```python
import jax
import jax.numpy as jnp
from jax import lax

NBLK = 12
BLOCK = 128
P_SIZE = 16
U = 48
VW = 1152
NB_ALL = 3072
DEVICES = 256


def draw_block_count(key, part):
    keyed = jax.random.fold_in(key, 7)
    counts = jax.random.randint(keyed, (DEVICES,), 1, max(2, 2 * NBLK // 3))
    chosen = jax.random.randint(jax.random.fold_in(keyed, 1), (), 0, DEVICES)
    return jnp.where(jnp.arange(DEVICES) == chosen, NBLK, counts).astype(jnp.int32)


def place_ends(result, own_key, low, largest):
    index_at = [jax.random.randint(jax.random.fold_in(own_key, axis), (), 0, length) for axis, length in enumerate(result.shape)]
    widest = result.shape.index(max(result.shape))
    neighbour = index_at[:widest] + [(index_at[widest] + 1) % result.shape[widest]] + index_at[widest + 1:]
    return result.at[tuple(index_at)].set(low).at[tuple(neighbour)].set(largest)


def raised(result, rng, source, target, shards_of, factor):
    owner, partner = [(jnp.arange(result.shape[position]) // (result.shape[position] // shards_of)).reshape([-1 if axis == position else 1 for axis in range(result.ndim)]) for position in (source, target)]
    chosen = jax.random.permutation(rng, shards_of)[partner]
    strong = (owner == chosen) | (owner == (partner + shards_of // 2) % shards_of)
    return jnp.where(strong, factor * result, result)


def level_of(rng, extent, cuts, smallest, high):
    gain = 1.0
    for position, blocks in cuts:
        heights = jax.random.uniform(jax.random.fold_in(jax.random.fold_in(rng, 6), position), (blocks,), jnp.float32, smallest / len(cuts), high / len(cuts))
        gain = gain * jnp.repeat(jnp.exp(heights), extent[position] // blocks).reshape((-1,) + (1,) * (len(extent) - 1 - position))
    return gain


def bell_draw(stream_key, shape, spread, limit, shards=(), kind=jnp.bfloat16):
    loudness = level_of(stream_key, shape, shards, -0.22, 0.18) if shards else 1.0
    result = jax.random.normal(stream_key, shape, jnp.float32) * spread * loudness
    return jnp.minimum(jnp.maximum(result, -limit), limit).astype(kind)


def gaussian_with(own_key, dims, deviation, most, cuts, heavy, kind=jnp.bfloat16):
    drawn = deviation * jax.random.normal(own_key, dims, jnp.float32)
    if cuts:
        drawn = drawn * level_of(own_key, dims, cuts, -0.22, 0.18)
    return jnp.clip(raised(drawn, jax.random.fold_in(own_key, 3), *heavy), -most, most).astype(kind)


def setup_inputs(seed: int = 0) -> dict:
    streams_of = jax.random.split(jax.random.key(seed), 6)
    return {
        "integrals": gaussian_with(streams_of[0], (NB_ALL, 2, BLOCK, VW), 1.0, 24.0, ((0, 256),), (0, 3, 128, 5.5)),
        "bra_rows": bell_draw(streams_of[1], (NB_ALL, 2, BLOCK, P_SIZE), (DEVICES * NBLK * BLOCK) ** -0.5, 0.009765625, ((0, 256),)),
        "ket_rows": bell_draw(streams_of[2], (NB_ALL, 2, BLOCK, U), 1.0, 6.0, ((0, 256),)),
        "block_count": draw_block_count(jax.random.fold_in(streams_of[5], 71), 0),
        "pair_count": place_ends(jax.random.randint(streams_of[4], (NB_ALL,), BLOCK // 4, BLOCK + 1), jax.random.fold_in(streams_of[4], 1), BLOCK // 4, BLOCK).astype(jnp.int32),
    }


def block_product(ints_block, bra_block, ket_block):
    bra_wide = bra_block.astype(jnp.float32)
    ket_wide = ket_block.astype(jnp.float32)
    real_part = bra_wide[0][:, :, None] * ket_wide[0][:, None, :] + bra_wide[1][:, :, None] * ket_wide[1][:, None, :]
    imag_part = bra_wide[0][:, :, None] * ket_wide[1][:, None, :] - bra_wide[1][:, :, None] * ket_wide[0][:, None, :]
    rows = bra_block.shape[1]
    real_low = real_part.reshape(rows, -1).T.astype(jnp.bfloat16)
    imag_low = imag_part.reshape(rows, -1).T.astype(jnp.bfloat16)
    upper = jnp.concatenate([real_low, -imag_low], axis=1)
    lower = jnp.concatenate([imag_low, real_low], axis=1)
    weights = jnp.concatenate([upper, lower], axis=0)
    stacked = ints_block.reshape(2 * rows, -1)
    return jnp.dot(weights, stacked, preferred_element_type=jnp.float32)


def reference(integrals, bra_rows, ket_rows, block_count, pair_count):
    slots_all = integrals.shape[0]
    per_device = slots_all // block_count.shape[0]
    positions = jnp.arange(slots_all, dtype=jnp.int32)
    owners = positions // per_device
    alive = (positions % per_device) < block_count[owners]
    pair_mask = (jnp.arange(BLOCK, dtype=jnp.int32)[None, :] < pair_count[:, None]).astype(jnp.bfloat16)
    order = jnp.argsort(1 - alive.astype(jnp.int32), stable=True).astype(jnp.int32)
    live_total = jnp.sum(alive.astype(jnp.int32))
    init = jnp.zeros((2 * P_SIZE * U, VW), jnp.float32)

    def accumulate(step_number, totals):
        chosen = order[step_number]
        ints_block = lax.dynamic_index_in_dim(integrals, chosen, 0, keepdims=False)
        bra_block = lax.dynamic_index_in_dim(bra_rows, chosen, 0, keepdims=False)
        ket_block = lax.dynamic_index_in_dim(ket_rows, chosen, 0, keepdims=False)
        mask_row = lax.dynamic_index_in_dim(pair_mask, chosen, 0, keepdims=False)
        ket_block = ket_block * mask_row[None, :, None]
        return totals + block_product(ints_block, bra_block, ket_block)

    totals = lax.fori_loop(0, live_total, accumulate, init)
    return totals.reshape(2, P_SIZE, U, VW)
```

```python
import jax
import jax.numpy as jnp
from jax import lax
from jax.experimental import pallas as pl
from jax.experimental.pallas import tpu as pltpu
from jax.sharding import PartitionSpec as P

MESH = pl.DeviceIdType.MESH
NBLK = 12
DEPTH = 256
VW = 1152
ROWS = 96
WIDE = 640
MSG = 48


def kernel(ints_hbm, bra_ref, ket_ref, block_count, pair_count, out_ref,
           ints, weights, psend, precv, s1, r1, s2, r2, turned, s3, r3,
           load_sem, p_send, p_recv, s1_send, s1_recv, s2_send, s2_recv, s3_send, s3_recv):
    ao, gen, act = lax.axis_index("ao"), lax.axis_index("gen"), lax.axis_index("act")
    core = ao % 2
    z = (ao // 2) % 8
    x_lo = ao // 16
    x_hi = act
    x = 2 * x_hi + x_lo
    y = gen

    def device(xx, yy, zz, cc):
        return (((xx % 2) * 8 + zz) * 2 + cc, yy, xx // 2)

    def first(d):
        return device(core * x + (1 - core) * d, core * d + (1 - core) * y, z, core)

    def second(d):
        return device(core * d + (1 - core) * x, core * y + (1 - core) * d, z, core)

    me1 = (1 - core) * x + core * y
    me2 = (1 - core) * y + core * x

    loads = []
    for b in range(NBLK):
        rows = pl.ds(b * DEPTH, DEPTH)
        loads.append(pltpu.make_async_copy(ints_hbm.at[rows], ints.at[rows], load_sem.at[b]))
        loads[-1].start()

    barrier = pltpu.get_barrier_semaphore()
    pl.semaphore_signal(barrier, inc=1, device_id=device(x, y, z, 1 - core), device_id_type=MESH)
    for k in (1, 2, 3):
        pl.semaphore_signal(barrier, inc=1, device_id=first((me1 + k) % 4), device_id_type=MESH)
        pl.semaphore_signal(barrier, inc=1, device_id=second((me2 + k) % 4), device_id_type=MESH)
    for k in range(1, 8):
        for c in (0, 1):
            pl.semaphore_signal(barrier, inc=1, device_id=device(x, y, (z + k) % 8, c), device_id_type=MESH)

    lane = lax.broadcasted_iota(jnp.int32, (48, 128), 1)
    eye16 = (lax.broadcasted_iota(jnp.int32, (16, 16), 0) == lax.broadcasted_iota(jnp.int32, (16, 16), 1)).astype(jnp.bfloat16)
    eye48 = (lax.broadcasted_iota(jnp.int32, (48, 48), 0) == lax.broadcasted_iota(jnp.int32, (48, 48), 1)).astype(jnp.bfloat16)

    def flipped(eye, block):
        return lax.dot_general(eye, block, (((1,), (1,)), ((), ())), preferred_element_type=jnp.float32)

    live_blocks = block_count[0]

    def build(b, carry):
        live = jnp.where(b < live_blocks, pair_count[b], 0)
        keep = lane < live
        bra_re = flipped(eye16, bra_ref[b, 0])
        bra_im = flipped(eye16, bra_ref[b, 1])
        ket_re = jnp.where(keep, flipped(eye48, ket_ref[b, 0]), 0.0)
        ket_im = jnp.where(keep, flipped(eye48, ket_ref[b, 1]), 0.0)
        low = pl.ds(pl.multiple_of(b * DEPTH, DEPTH), 128)
        high = pl.ds(pl.multiple_of(b * DEPTH + 128, 128), 128)
        for xh in (0, 1):
            kr = ket_re[xh * 24 : xh * 24 + 24]
            ki = ket_im[xh * 24 : xh * 24 + 24]
            for yy in range(4):
                re, im = [], []
                for p in range(4):
                    br = bra_re[yy * 4 + p : yy * 4 + p + 1]
                    bi = bra_im[yy * 4 + p : yy * 4 + p + 1]
                    re.append(br * kr + bi * ki)
                    im.append(br * ki - bi * kr)
                re = jnp.concatenate(re, axis=0)
                im = jnp.concatenate(im, axis=0)
                re_low = re.astype(jnp.bfloat16)
                im_low = im.astype(jnp.bfloat16)
                weights[0, xh * 4 + yy, :, low] = re_low
                weights[0, xh * 4 + yy, :, high] = -im_low
                weights[1, yy * 2 + xh, :, low] = im_low
                weights[1, yy * 2 + xh, :, high] = re_low
        return carry

    lax.fori_loop(0, NBLK, build, 0)

    for copy in loads:
        copy.wait()

    other_x = 1 - x_hi

    def chunk_of(part, t):
        from_x = (other_x if t < 2 else x_hi) * 2 + t % 2
        from_y = (y + (2, 1, 3, 0)[t]) % 4
        return (1 - part) * from_x + part * from_y

    def product(part, chunk):
        lhs = weights[part, pl.ds(chunk * 2, 2)].reshape(2 * ROWS, NBLK * DEPTH)
        return jnp.dot(lhs, ints[...], preferred_element_type=jnp.float32)

    def p_copy(t):
        return pltpu.make_async_remote_copy(
            src_ref=psend.at[t], dst_ref=precv.at[t], send_sem=p_send.at[t], recv_sem=p_recv.at[t],
            device_id=device(x, y, z, 1 - core), device_id_type=MESH)

    def for_partner(t):
        psend[t] = product(1 - core, chunk_of(1 - core, t)).astype(jnp.bfloat16)
        if t == 0:
            pl.semaphore_wait(barrier, 21)
        p_copy(t).start()

    def s1_target(t, a):
        d1 = (1 - core) * (2 * (other_x if t < 2 else x_hi) + a) + core * chunk_of(1, t)
        half = (1 - core) * (t % 2) + core * a
        return d1, half

    def s1_copy(t, a):
        d1, half = s1_target(t, a)
        slot = (me1 - d1 + 7) % 4
        return pltpu.make_async_remote_copy(
            src_ref=s1.at[d1, half], dst_ref=r1.at[slot % 3, half],
            send_sem=s1_send.at[t, a], recv_sem=s1_recv.at[slot % 3, half],
            device_id=first(d1), device_id_type=MESH)

    def for_self(t):
        value = product(core, chunk_of(core, t))
        p_copy(t).wait_recv()
        value = value + precv[t].astype(jnp.float32)
        low = value.astype(jnp.bfloat16)
        for j in (0, 1):
            for xl in (0, 1):
                d1 = (1 - core) * (2 * (other_x if t < 2 else x_hi) + xl) + core * chunk_of(1, t)
                d2 = (1 - core) * (2 * (t % 2) + j) + core * (2 * j + xl)
                s1[d1, d2 // 2, d2 % 2] = low[j * ROWS : (j + 1) * ROWS, xl * 512 : xl * 512 + WIDE]
        for a in (0, 1):
            d1, _ = s1_target(t, a)

            @pl.when(d1 != me1)
            def _():
                s1_copy(t, a).start()

    for_partner(0)
    for_partner(1)
    for_self(0)
    for_partner(2)
    for_self(1)
    for_partner(3)
    for_self(2)
    for_self(3)

    def s1_arrival(slot, half):
        return pltpu.make_async_remote_copy(
            src_ref=s1.at[0, half], dst_ref=r1.at[slot, half],
            send_sem=s1_send.at[0, 0], recv_sem=s1_recv.at[slot, half],
            device_id=first((me1 + 1) % 4), device_id_type=MESH)

    for slot in range(3):
        for half in (0, 1):
            s1_arrival(slot, half).wait_recv()

    def s2_copy(k):
        d2 = (me2 + k) % 4
        slot = 3 - k
        return pltpu.make_async_remote_copy(
            src_ref=s2.at[k - 1], dst_ref=r2.at[slot], send_sem=s2_send.at[k - 1], recv_sem=s2_recv.at[slot],
            device_id=second(d2), device_id_type=MESH)

    def summed(d2):
        half, side = d2 // 2, d2 % 2
        total = s1[me1, half, side].astype(jnp.float32)
        for slot in range(3):
            total = total + r1[slot, half, side].astype(jnp.float32)
        return total

    for k in (2, 1, 3):
        s2[k - 1] = summed((me2 + k) % 4).astype(jnp.bfloat16)
        s2_copy(k).start()
    total = summed(me2)
    for k in (1, 2, 3):
        s2_copy(k).wait_recv()
        total = total + r2[3 - k].astype(jnp.float32)

    pad = jnp.zeros((32, 128), jnp.float32)
    for tile in range(5):
        turned[tile * 128 : (tile + 1) * 128] = jnp.concatenate([total[:, tile * 128 : (tile + 1) * 128], pad], axis=0).T
    turned[WIDE:] = jnp.zeros((16, 128), jnp.float32)

    def s3_copy(k, c):
        zz = (z + k) % 8
        return pltpu.make_async_remote_copy(
            src_ref=s3.at[zz, c], dst_ref=r3.at[core, z], send_sem=s3_send.at[k, c], recv_sem=s3_recv.at[core, z],
            device_id=device(x, y, zz, c), device_id_type=MESH)

    for k in (4, 3, 5, 2, 6, 1, 7, 0):
        zz = (z + k) % 8
        for c in (0, 1):
            start = pl.multiple_of(64 * x_lo + 72 * zz + 32 * c, 8)
            s3[zz, c] = turned[pl.ds(start, MSG)].astype(jnp.bfloat16)
            if k > 0:
                s3_copy(k, c).start()
            else:

                @pl.when(core != c)
                def _():
                    s3_copy(k, c).start()

    r3[core, z] = s3[z, core]
    for k in range(8):
        zz = (z + k) % 8
        for c in (0, 1):

            def arrival():
                return pltpu.make_async_remote_copy(
                    src_ref=s3.at[0, 0], dst_ref=r3.at[c, zz], send_sem=s3_send.at[0, 0], recv_sem=s3_recv.at[c, zz],
                    device_id=device(x, y, z, 1 - core), device_id_type=MESH)

            if k > 0:
                arrival().wait_recv()
            else:

                @pl.when(core != c)
                def _():
                    arrival().wait_recv()

    fill = jnp.zeros((128 - MSG, 128), jnp.float32)
    for r in (0, 1):
        piece = r3[r, 0].astype(jnp.float32)
        for zz in range(1, 8):
            piece = piece + r3[r, zz].astype(jnp.float32)
        back = jnp.concatenate([piece, fill], axis=0).T
        out_ref[r] = jnp.where(core == 0, back[:ROWS, :36], back[:ROWS, 4:40])

    for t in range(4):
        p_copy(t).wait_send()
        for a in (0, 1):
            d1, _ = s1_target(t, a)

            @pl.when(d1 != me1)
            def _():
                s1_copy(t, a).wait_send()
    for k in (1, 2, 3):
        s2_copy(k).wait_send()
    for k in range(8):
        for c in (0, 1):
            if k > 0:
                s3_copy(k, c).wait_send()
            else:

                @pl.when(core != c)
                def _():
                    s3_copy(k, c).wait_send()


def local(integrals, bra_rows, ket_rows, block_count, pair_count):
    bf16, f32 = jnp.bfloat16, jnp.float32
    out = pl.pallas_call(
        kernel,
        out_shape=jax.ShapeDtypeStruct((2, ROWS, 36), f32),
        in_specs=[
            pl.BlockSpec(memory_space=pl.ANY),
            pl.BlockSpec(memory_space=pltpu.VMEM),
            pl.BlockSpec(memory_space=pltpu.VMEM),
            pl.BlockSpec(memory_space=pltpu.SMEM),
            pl.BlockSpec(memory_space=pltpu.SMEM),
        ],
        out_specs=pl.BlockSpec(memory_space=pltpu.VMEM),
        scratch_shapes=[
            pltpu.VMEM((NBLK * DEPTH, VW), bf16),
            pltpu.VMEM((2, 8, ROWS, NBLK * DEPTH), bf16),
            pltpu.VMEM((4, 2 * ROWS, VW), bf16),
            pltpu.VMEM((4, 2 * ROWS, VW), bf16),
            pltpu.VMEM((4, 2, 2, ROWS, WIDE), bf16),
            pltpu.VMEM((3, 2, 2, ROWS, WIDE), bf16),
            pltpu.VMEM((3, ROWS, WIDE), bf16),
            pltpu.VMEM((3, ROWS, WIDE), bf16),
            pltpu.VMEM((WIDE + 16, 128), f32),
            pltpu.VMEM((8, 2, MSG, 128), bf16),
            pltpu.VMEM((2, 8, MSG, 128), bf16),
            pltpu.SemaphoreType.DMA((NBLK,)),
            pltpu.SemaphoreType.DMA((4,)),
            pltpu.SemaphoreType.DMA((4,)),
            pltpu.SemaphoreType.DMA((4, 2)),
            pltpu.SemaphoreType.DMA((3, 2)),
            pltpu.SemaphoreType.DMA((3,)),
            pltpu.SemaphoreType.DMA((3,)),
            pltpu.SemaphoreType.DMA((8, 2)),
            pltpu.SemaphoreType.DMA((2, 8)),
        ],
        compiler_params=pltpu.CompilerParams(
            collective_id=0, has_side_effects=True, vmem_limit_bytes=56 * 1024 * 1024
        ),
        name="transform",
    )(integrals.reshape(NBLK * DEPTH, VW), bra_rows, ket_rows, block_count, pair_count)
    return out.reshape(2, 4, 24, 36)


def solution(mesh):
    split = ("ao", "gen", "act")
    in_specs = (
        P(split, None, None, None),
        P(split, None, None, None),
        P(split, None, None, None),
        P(split),
        P(split),
    )
    out_specs = P(None, "gen", "act", "ao")
    return jax.shard_map(local, mesh=mesh, in_specs=in_specs, out_specs=out_specs, check_vma=False)
```

```python
import jax
import jax.numpy as jnp
from jax import lax
from jax.experimental import pallas as pl
from jax.experimental.pallas import tpu as pltpu
from jax.sharding import PartitionSpec as P

MESH = pl.DeviceIdType.MESH
NBLK = 12
DEPTH = 256
VW = 1152
ROWS = 96
WIDE = 640
MSG = 48


def kernel(ints_hbm, bra_ref, ket_ref, block_count, pair_count, out_ref,
           ints, bra_wide, ket_wide, weights, psend, precv, s1, r1, joined, s2, r2, mine, turned, s3, r3,
           load_sem, p_send, p_recv, s1_send, s1_recv, s2_send, s2_recv, s3_send, s3_recv):
    ao, gen, act = lax.axis_index("ao"), lax.axis_index("gen"), lax.axis_index("act")
    core = ao % 2
    z = (ao // 2) % 8
    x_lo = ao // 16
    x_hi = act
    x = 2 * x_hi + x_lo
    y = gen

    def device(xx, yy, zz, cc):
        return (((xx % 2) * 8 + zz) * 2 + cc, yy, xx // 2)

    def first(d):
        return device(core * x + (1 - core) * d, core * d + (1 - core) * y, z, core)

    def second(d):
        return device(core * d + (1 - core) * x, core * y + (1 - core) * d, z, core)

    me1 = (1 - core) * x + core * y
    me2 = (1 - core) * y + core * x

    loads = []
    for b in range(NBLK):
        rows = pl.ds(b * DEPTH, DEPTH)
        loads.append(pltpu.make_async_copy(ints_hbm.at[rows], ints.at[rows], load_sem.at[b]))
        loads[-1].start()

    barrier = pltpu.get_barrier_semaphore()
    pl.semaphore_signal(barrier, inc=1, device_id=device(x, y, z, 1 - core), device_id_type=MESH)
    for k in (1, 2, 3):
        pl.semaphore_signal(barrier, inc=1, device_id=first((me1 + k) % 4), device_id_type=MESH)
        pl.semaphore_signal(barrier, inc=1, device_id=second((me2 + k) % 4), device_id_type=MESH)
    for k in range(1, 8):
        for c in (0, 1):
            pl.semaphore_signal(barrier, inc=1, device_id=device(x, y, (z + k) % 8, c), device_id_type=MESH)

    lane = lax.broadcasted_iota(jnp.int32, (48, 128), 1)
    live_blocks = block_count[0]

    def build(b, carry):
        live = jnp.where(b < live_blocks, pair_count[b], 0)
        keep = lane < live
        for r in (0, 1):
            bra_wide[r] = bra_ref[b, r].astype(jnp.float32)
            ket_wide[r] = jnp.where(keep, ket_ref[b, r].astype(jnp.float32), 0.0)
        low = pl.ds(pl.multiple_of(b * DEPTH, DEPTH), 128)
        high = pl.ds(pl.multiple_of(b * DEPTH + 128, 128), 128)
        for xh in (0, 1):
            kr = ket_wide[0, xh * 24 : xh * 24 + 24]
            ki = ket_wide[1, xh * 24 : xh * 24 + 24]
            for yy in range(4):
                re, im = [], []
                for p in range(4):
                    br = bra_wide[0, yy * 4 + p : yy * 4 + p + 1]
                    bi = bra_wide[1, yy * 4 + p : yy * 4 + p + 1]
                    re.append(br * kr + bi * ki)
                    im.append(br * ki - bi * kr)
                re = jnp.concatenate(re, axis=0)
                im = jnp.concatenate(im, axis=0)
                re_low = re.astype(jnp.bfloat16)
                im_low = im.astype(jnp.bfloat16)
                weights[0, xh * 4 + yy, :, low] = re_low
                weights[0, xh * 4 + yy, :, high] = -im_low
                weights[1, yy * 2 + xh, :, low] = im_low
                weights[1, yy * 2 + xh, :, high] = re_low
        return carry

    lax.fori_loop(0, NBLK, build, 0)

    for copy in loads:
        copy.wait()

    other_x = 1 - x_hi

    def chunk_of(part, t):
        from_x = (other_x if t < 2 else x_hi) * 2 + t % 2
        from_y = (y + (2, 1, 3, 0)[t]) % 4
        return (1 - part) * from_x + part * from_y

    def product(part, chunk):
        lhs = weights[part, pl.ds(chunk * 2, 2)].reshape(2 * ROWS, NBLK * DEPTH)
        return jnp.dot(lhs, ints[...], preferred_element_type=jnp.float32)

    def p_copy(t):
        return pltpu.make_async_remote_copy(
            src_ref=psend.at[t], dst_ref=precv.at[t], send_sem=p_send.at[t], recv_sem=p_recv.at[t],
            device_id=device(x, y, z, 1 - core), device_id_type=MESH)

    def for_partner(t):
        psend[t] = product(1 - core, chunk_of(1 - core, t)).astype(jnp.bfloat16)
        if t == 0:
            pl.semaphore_wait(barrier, 21)
        p_copy(t).start()

    right, left = (me1 + 1) % 4, (me1 + 3) % 4
    side = {0: right, 1: left}

    def remote1(src_ref, dst_ref, k, to):
        return pltpu.make_async_remote_copy(
            src_ref=src_ref, dst_ref=dst_ref, send_sem=s1_send.at[k], recv_sem=s1_recv.at[k],
            device_id=first(side[to]), device_id_type=MESH)

    def opposite(to):
        return remote1(s1.at[(me1 + 2) % 4, to], r1.at[to], to, to)

    def plain(to):
        return remote1(s1.at[side[to], 1 - to], r1.at[2 + to], 2 + to, to)

    def relayed(to):
        return remote1(joined.at[to], r1.at[4 + to], 4 + to, to)

    def relay(to):
        opposite(to).wait_recv()
        for j in (0, 1):
            joined[to, j] = (s1[side[to], to, j].astype(jnp.float32) + r1[to, j].astype(jnp.float32)).astype(jnp.bfloat16)
        relayed(to).start()

    def for_self(t):
        p_copy(t).wait_recv()
        value = product(core, chunk_of(core, t)) + precv[t].astype(jnp.float32)
        low = value.astype(jnp.bfloat16)
        for j in (0, 1):
            for xl in (0, 1):
                d1 = (1 - core) * (2 * (other_x if t < 2 else x_hi) + xl) + core * chunk_of(1, t)
                d2 = (1 - core) * (2 * (t % 2) + j) + core * (2 * j + xl)
                s1[d1, d2 // 2, d2 % 2] = low[j * ROWS : (j + 1) * ROWS, xl * 512 : xl * 512 + WIDE]

    is_y = core == 1
    even = jnp.logical_and(core == 0, x_lo == 0)
    odd = jnp.logical_and(core == 0, x_lo == 1)

    def when(*conditions):
        condition = conditions[0]
        for extra in conditions[1:]:
            condition = jnp.logical_or(condition, extra)
        return pl.when(condition)

    for_partner(0)
    for_partner(1)
    for_self(0)
    opposite(0).start()

    @when(is_y)
    def _():
        opposite(1).start()

    @when(even)
    def _():
        plain(1).start()

    for_partner(2)
    for_self(1)

    @when(even, odd)
    def _():
        opposite(1).start()

    @when(is_y, odd)
    def _():
        plain(0).start()
        relay(0)

    for_partner(3)
    for_self(2)

    @when(is_y, odd)
    def _():
        plain(1).start()

    @when(even)
    def _():
        relay(0)

    @when(is_y, even)
    def _():
        relay(1)

    for_self(3)

    @when(even)
    def _():
        plain(0).start()

    @when(odd)
    def _():
        relay(1)

    def s2_copy(d2, slot):
        return pltpu.make_async_remote_copy(
            src_ref=s2.at[d2], dst_ref=r2.at[slot], send_sem=s2_send.at[d2], recv_sem=s2_recv.at[slot],
            device_id=second(d2), device_id_type=MESH)

    for half in (0, 1):
        relayed(half).wait_recv()
        plain(1 - half).wait_recv()
        for j in (0, 1):
            d2 = 2 * half + j
            total = s1[me1, half, j].astype(jnp.float32) + r1[4 + half, j].astype(jnp.float32) + r1[3 - half, j].astype(jnp.float32)
            s2[d2] = total.astype(jnp.bfloat16)

            @pl.when(d2 == me2)
            def _():
                mine[...] = total

            @pl.when(d2 != me2)
            def _():
                s2_copy(d2, (me2 - d2 + 7) % 4 % 3).start()

    for slot in range(3):
        s2_copy(0, slot).wait_recv()
    total = mine[...]
    for slot in range(3):
        total = total + r2[slot].astype(jnp.float32)

    pad = jnp.zeros((32, 128), jnp.float32)
    for tile in range(5):
        turned[tile * 128 : (tile + 1) * 128] = jnp.concatenate([total[:, tile * 128 : (tile + 1) * 128], pad], axis=0).T
    turned[WIDE:] = jnp.zeros((16, 128), jnp.float32)

    def s3_copy(k, c):
        zz = (z + k) % 8
        return pltpu.make_async_remote_copy(
            src_ref=s3.at[zz, c], dst_ref=r3.at[core, z], send_sem=s3_send.at[k, c], recv_sem=s3_recv.at[core, z],
            device_id=device(x, y, zz, c), device_id_type=MESH)

    for k in (4, 3, 5, 2, 6, 1, 7, 0):
        zz = (z + k) % 8
        for c in (0, 1):
            start = pl.multiple_of(64 * x_lo + 72 * zz + 32 * c, 8)
            s3[zz, c] = turned[pl.ds(start, MSG)].astype(jnp.bfloat16)
            if k > 0:
                s3_copy(k, c).start()
            else:

                @pl.when(core != c)
                def _():
                    s3_copy(k, c).start()

    r3[core, z] = s3[z, core]
    for k in range(8):
        zz = (z + k) % 8
        for c in (0, 1):

            def arrival():
                return pltpu.make_async_remote_copy(
                    src_ref=s3.at[0, 0], dst_ref=r3.at[c, zz], send_sem=s3_send.at[0, 0], recv_sem=s3_recv.at[c, zz],
                    device_id=device(x, y, z, 1 - core), device_id_type=MESH)

            if k > 0:
                arrival().wait_recv()
            else:

                @pl.when(core != c)
                def _():
                    arrival().wait_recv()

    fill = jnp.zeros((128 - MSG, 128), jnp.float32)
    for r in (0, 1):
        piece = r3[r, 0].astype(jnp.float32)
        for zz in range(1, 8):
            piece = piece + r3[r, zz].astype(jnp.float32)
        back = jnp.concatenate([piece, fill], axis=0).T
        out_ref[r] = jnp.where(core == 0, back[:ROWS, :36], back[:ROWS, 4:40])

    for t in range(4):
        p_copy(t).wait_send()
    for to in (0, 1):
        opposite(to).wait_send()
        plain(to).wait_send()
        relayed(to).wait_send()
    for d2 in range(4):

        @pl.when(d2 != me2)
        def _():
            s2_copy(d2, 0).wait_send()

    for k in range(8):
        for c in (0, 1):
            if k > 0:
                s3_copy(k, c).wait_send()
            else:

                @pl.when(core != c)
                def _():
                    s3_copy(k, c).wait_send()


def local(integrals, bra_rows, ket_rows, block_count, pair_count):
    bf16, f32 = jnp.bfloat16, jnp.float32
    out = pl.pallas_call(
        kernel,
        out_shape=jax.ShapeDtypeStruct((2, ROWS, 36), f32),
        in_specs=[
            pl.BlockSpec(memory_space=pl.ANY),
            pl.BlockSpec(memory_space=pltpu.VMEM),
            pl.BlockSpec(memory_space=pltpu.VMEM),
            pl.BlockSpec(memory_space=pltpu.SMEM),
            pl.BlockSpec(memory_space=pltpu.SMEM),
        ],
        out_specs=pl.BlockSpec(memory_space=pltpu.VMEM),
        scratch_shapes=[
            pltpu.VMEM((NBLK * DEPTH, VW), bf16),
            pltpu.VMEM((2, 16, 128), f32),
            pltpu.VMEM((2, 48, 128), f32),
            pltpu.VMEM((2, 8, ROWS, NBLK * DEPTH), bf16),
            pltpu.VMEM((4, 2 * ROWS, VW), bf16),
            pltpu.VMEM((4, 2 * ROWS, VW), bf16),
            pltpu.VMEM((4, 2, 2, ROWS, WIDE), bf16),
            pltpu.VMEM((6, 2, ROWS, WIDE), bf16),
            pltpu.VMEM((2, 2, ROWS, WIDE), bf16),
            pltpu.VMEM((4, ROWS, WIDE), bf16),
            pltpu.VMEM((3, ROWS, WIDE), bf16),
            pltpu.VMEM((ROWS, WIDE), f32),
            pltpu.VMEM((WIDE + 16, 128), f32),
            pltpu.VMEM((8, 2, MSG, 128), bf16),
            pltpu.VMEM((2, 8, MSG, 128), bf16),
            pltpu.SemaphoreType.DMA((NBLK,)),
            pltpu.SemaphoreType.DMA((4,)),
            pltpu.SemaphoreType.DMA((4,)),
            pltpu.SemaphoreType.DMA((6,)),
            pltpu.SemaphoreType.DMA((6,)),
            pltpu.SemaphoreType.DMA((4,)),
            pltpu.SemaphoreType.DMA((3,)),
            pltpu.SemaphoreType.DMA((8, 2)),
            pltpu.SemaphoreType.DMA((2, 8)),
        ],
        compiler_params=pltpu.CompilerParams(
            collective_id=0, has_side_effects=True, vmem_limit_bytes=56 * 1024 * 1024
        ),
        name="transform",
    )(integrals.reshape(NBLK * DEPTH, VW), jnp.swapaxes(bra_rows, 2, 3), jnp.swapaxes(ket_rows, 2, 3), block_count, pair_count)
    return out.reshape(2, 4, 24, 36)


def solution(mesh):
    split = ("ao", "gen", "act")
    in_specs = (
        P(split, None, None, None),
        P(split, None, None, None),
        P(split, None, None, None),
        P(split),
        P(split),
    )
    out_specs = P(None, "gen", "act", "ao")
    return jax.shard_map(local, mesh=mesh, in_specs=in_specs, out_specs=out_specs, check_vma=False)
```

```python
import jax
import jax.numpy as jnp
from jax import lax
from jax.experimental import pallas as pl
from jax.experimental.pallas import tpu as pltpu
from jax.sharding import PartitionSpec as P

MESH = pl.DeviceIdType.MESH
NBLK = 12
DEPTH = 256
VW = 1152
ROWS = 96
HALF = 48
WIDE = 640
MSG = 48


def kernel(ints_hbm, bra_ref, ket_ref, block_count, pair_count, out_ref,
           ints, bra_wide, ket_wide, weights, psend, precv, s1, r1, joined, s2, r2, mine, turned, s3, r3,
           load_sem, p_send, p_recv, s1_send, s1_recv, s2_send, s2_recv, s3_send, s3_recv):
    ao, gen, act = lax.axis_index("ao"), lax.axis_index("gen"), lax.axis_index("act")
    core = ao % 2
    z = (ao // 2) % 8
    x_lo = ao // 16
    x_hi = act
    x = 2 * x_hi + x_lo
    y = gen

    def device(xx, yy, zz, cc):
        return (((xx % 2) * 8 + zz) * 2 + cc, yy, xx // 2)

    def first(d):
        return device(core * x + (1 - core) * d, core * d + (1 - core) * y, z, core)

    def second(d):
        return device(core * d + (1 - core) * x, core * y + (1 - core) * d, z, core)

    me1 = (1 - core) * x + core * y
    me2 = (1 - core) * y + core * x

    loads = []
    for b in range(NBLK):
        rows = pl.ds(b * DEPTH, DEPTH)
        loads.append(pltpu.make_async_copy(ints_hbm.at[rows], ints.at[rows], load_sem.at[b]))
        loads[-1].start()

    barrier = pltpu.get_barrier_semaphore()
    pl.semaphore_signal(barrier, inc=1, device_id=device(x, y, z, 1 - core), device_id_type=MESH)
    for k in (1, 2, 3):
        pl.semaphore_signal(barrier, inc=1, device_id=first((me1 + k) % 4), device_id_type=MESH)
        pl.semaphore_signal(barrier, inc=1, device_id=second((me2 + k) % 4), device_id_type=MESH)
    for k in range(1, 8):
        for c in (0, 1):
            pl.semaphore_signal(barrier, inc=1, device_id=device(x, y, (z + k) % 8, c), device_id_type=MESH)

    lane = lax.broadcasted_iota(jnp.int32, (48, 128), 1)
    live_blocks = block_count[0]

    def build(b, carry):
        live = jnp.where(b < live_blocks, pair_count[b], 0)
        keep = lane < live
        for r in (0, 1):
            bra_wide[r] = bra_ref[b, r].astype(jnp.float32)
            ket_wide[r] = jnp.where(keep, ket_ref[b, r].astype(jnp.float32), 0.0)
        low = pl.ds(pl.multiple_of(b * DEPTH, DEPTH), 128)
        high = pl.ds(pl.multiple_of(b * DEPTH + 128, 128), 128)
        for xh in (0, 1):
            kr = ket_wide[0, xh * 24 : xh * 24 + 24]
            ki = ket_wide[1, xh * 24 : xh * 24 + 24]
            for yy in range(4):
                for ab in (0, 1):
                    re, im = [], []
                    for p in (2 * ab, 2 * ab + 1):
                        br = bra_wide[0, yy * 4 + p : yy * 4 + p + 1]
                        bi = bra_wide[1, yy * 4 + p : yy * 4 + p + 1]
                        re.append(br * kr + bi * ki)
                        im.append(br * ki - bi * kr)
                    re_low = jnp.concatenate(re, axis=0).astype(jnp.bfloat16)
                    im_low = jnp.concatenate(im, axis=0).astype(jnp.bfloat16)
                    rows_x = pl.ds((yy % 2) * HALF, HALF)
                    rows_y = pl.ds(xh * HALF, HALF)
                    weights[0, ab, xh * 2 + yy // 2, rows_x, low] = re_low
                    weights[0, ab, xh * 2 + yy // 2, rows_x, high] = -im_low
                    weights[1, ab, yy, rows_y, low] = im_low
                    weights[1, ab, yy, rows_y, high] = re_low
        return carry

    lax.fori_loop(0, NBLK, build, 0)

    for copy in loads:
        copy.wait()

    to1 = 1 - me1 % 2
    to2 = 1 - to1

    def side(to):
        return (me1 + 1 + 2 * to) % 4

    def groups(part, sub):
        from_x = 2 * (x_hi if sub else 1 - x_hi)
        near = (y + 1 + 2 * (1 - y % 2)) % 4
        far = (y + 1 + 2 * (y % 2)) % 4
        from_y = (far, y) if sub else ((y + 2) % 4, near)
        return [(1 - part) * (from_x + j) + part * from_y[j] for j in (0, 1)]

    def product(part, ab, sub):
        lhs = jnp.concatenate([weights[part, ab, g] for g in groups(part, sub)], axis=0)
        return jnp.dot(lhs, ints[...], preferred_element_type=jnp.float32)

    def p_copy(ab, sub):
        k = 2 * ab + sub
        return pltpu.make_async_remote_copy(
            src_ref=psend.at[k], dst_ref=precv.at[k], send_sem=p_send.at[k], recv_sem=p_recv.at[k],
            device_id=device(x, y, z, 1 - core), device_id_type=MESH)

    def for_partner(ab, sub):
        psend[2 * ab + sub] = product(1 - core, ab, sub).astype(jnp.bfloat16)
        if ab == 0 and sub == 0:
            pl.semaphore_wait(barrier, 21)
        p_copy(ab, sub).start()

    def for_self(ab, sub):
        p_copy(ab, sub).wait_recv()
        value = product(core, ab, sub) + precv[2 * ab + sub].astype(jnp.float32)
        low = value.astype(jnp.bfloat16)
        from_x = 2 * (x_hi if sub else 1 - x_hi)
        for j, g in enumerate(groups(core, sub)):
            for i in (0, 1):
                for xl in (0, 1):
                    d1 = (1 - core) * (from_x + xl) + core * g
                    half = (1 - core) * j + core * i
                    spot = (1 - core) * i + core * xl
                    row = (2 * j + i) * HALF
                    s1[ab, d1, half, spot] = low[row : row + HALF, xl * 512 : xl * 512 + WIDE]

    def remote1(src_ref, ab, k, to):
        return pltpu.make_async_remote_copy(
            src_ref=src_ref, dst_ref=r1.at[ab, k], send_sem=s1_send.at[ab, k], recv_sem=s1_recv.at[ab, k],
            device_id=first(side(to)), device_id_type=MESH)

    def opposite(ab, to):
        return remote1(s1.at[ab, (me1 + 2) % 4, to], ab, to, to)

    def plain(ab, to):
        return remote1(s1.at[ab, side(to), 1 - to], ab, 2 + to, to)

    def relayed(ab, to):
        return remote1(joined.at[ab, to], ab, 4 + to, to)

    def relay(ab, to):
        opposite(ab, to).wait_recv()
        for j in (0, 1):
            joined[ab, to, j] = (
                s1[ab, side(to), to, j].astype(jnp.float32) + r1[ab, to, j].astype(jnp.float32)
            ).astype(jnp.bfloat16)
        relayed(ab, to).start()

    def s2_copy(ab, d2, slot):
        return pltpu.make_async_remote_copy(
            src_ref=s2.at[ab, d2], dst_ref=r2.at[ab, slot], send_sem=s2_send.at[ab, d2], recv_sem=s2_recv.at[ab, slot],
            device_id=second(d2), device_id_type=MESH)

    def second_stage(ab):
        for half in (0, 1):
            relayed(ab, half).wait_recv()
            plain(ab, 1 - half).wait_recv()
            for j in (0, 1):
                d2 = 2 * half + j
                total = (
                    s1[ab, me1, half, j].astype(jnp.float32)
                    + r1[ab, 4 + half, j].astype(jnp.float32)
                    + r1[ab, 3 - half, j].astype(jnp.float32)
                )
                s2[ab, d2] = total.astype(jnp.bfloat16)

                @pl.when(d2 == me2)
                def _():
                    mine[ab] = total

                @pl.when(d2 != me2)
                def _():
                    s2_copy(ab, d2, (me2 - d2 + 7) % 4 % 3).start()

    def collected(ab):
        for slot in range(3):
            s2_copy(ab, 0, slot).wait_recv()
        total = mine[ab]
        for slot in range(3):
            total = total + r2[ab, slot].astype(jnp.float32)
        return total

    def out_first(ab):
        opposite(ab, to1).start()
        opposite(ab, to2).start()
        plain(ab, to1).start()

    for_partner(0, 0)
    for_partner(0, 1)
    for_self(0, 0)
    out_first(0)
    for_partner(1, 0)
    for_self(0, 1)
    plain(0, to2).start()
    relay(0, to1)
    relay(0, to2)
    for_partner(1, 1)
    for_self(1, 0)
    out_first(1)
    for_self(1, 1)
    plain(1, to2).start()
    second_stage(0)
    relay(1, to1)
    relay(1, to2)
    early = collected(0)
    second_stage(1)
    total = jnp.concatenate([early, collected(1)], axis=0)

    pad = jnp.zeros((32, 128), jnp.float32)
    for tile in range(5):
        turned[tile * 128 : (tile + 1) * 128] = jnp.concatenate([total[:, tile * 128 : (tile + 1) * 128], pad], axis=0).T
    turned[WIDE:] = jnp.zeros((16, 128), jnp.float32)

    def s3_copy(k, c):
        zz = (z + k) % 8
        return pltpu.make_async_remote_copy(
            src_ref=s3.at[zz, c], dst_ref=r3.at[core, z], send_sem=s3_send.at[k, c], recv_sem=s3_recv.at[core, z],
            device_id=device(x, y, zz, c), device_id_type=MESH)

    for k in (4, 3, 5, 2, 6, 1, 7, 0):
        zz = (z + k) % 8
        for c in (0, 1):
            start = pl.multiple_of(64 * x_lo + 72 * zz + 32 * c, 8)
            s3[zz, c] = turned[pl.ds(start, MSG)].astype(jnp.bfloat16)
            if k > 0:
                s3_copy(k, c).start()
            else:

                @pl.when(core != c)
                def _():
                    s3_copy(k, c).start()

    r3[core, z] = s3[z, core]
    for k in range(8):
        zz = (z + k) % 8
        for c in (0, 1):

            def arrival():
                return pltpu.make_async_remote_copy(
                    src_ref=s3.at[0, 0], dst_ref=r3.at[c, zz], send_sem=s3_send.at[0, 0], recv_sem=s3_recv.at[c, zz],
                    device_id=device(x, y, z, 1 - core), device_id_type=MESH)

            if k > 0:
                arrival().wait_recv()
            else:

                @pl.when(core != c)
                def _():
                    arrival().wait_recv()

    fill = jnp.zeros((128 - MSG, 128), jnp.float32)
    for r in (0, 1):
        piece = r3[r, 0].astype(jnp.float32)
        for zz in range(1, 8):
            piece = piece + r3[r, zz].astype(jnp.float32)
        back = jnp.concatenate([piece, fill], axis=0).T
        out_ref[r] = jnp.where(core == 0, back[:ROWS, :36], back[:ROWS, 4:40])

    for ab in (0, 1):
        for sub in (0, 1):
            p_copy(ab, sub).wait_send()
            opposite(ab, sub).wait_send()
            plain(ab, sub).wait_send()
            relayed(ab, sub).wait_send()
        for d2 in range(4):

            @pl.when(d2 != me2)
            def _():
                s2_copy(ab, d2, 0).wait_send()

    for k in range(8):
        for c in (0, 1):
            if k > 0:
                s3_copy(k, c).wait_send()
            else:

                @pl.when(core != c)
                def _():
                    s3_copy(k, c).wait_send()


def local(integrals, bra_rows, ket_rows, block_count, pair_count):
    bf16, f32 = jnp.bfloat16, jnp.float32
    out = pl.pallas_call(
        kernel,
        out_shape=jax.ShapeDtypeStruct((2, ROWS, 36), f32),
        in_specs=[
            pl.BlockSpec(memory_space=pl.ANY),
            pl.BlockSpec(memory_space=pltpu.VMEM),
            pl.BlockSpec(memory_space=pltpu.VMEM),
            pl.BlockSpec(memory_space=pltpu.SMEM),
            pl.BlockSpec(memory_space=pltpu.SMEM),
        ],
        out_specs=pl.BlockSpec(memory_space=pltpu.VMEM),
        scratch_shapes=[
            pltpu.VMEM((NBLK * DEPTH, VW), bf16),
            pltpu.VMEM((2, 16, 128), f32),
            pltpu.VMEM((2, 48, 128), f32),
            pltpu.VMEM((2, 2, 4, ROWS, NBLK * DEPTH), bf16),
            pltpu.VMEM((4, 2 * ROWS, VW), bf16),
            pltpu.VMEM((4, 2 * ROWS, VW), bf16),
            pltpu.VMEM((2, 4, 2, 2, HALF, WIDE), bf16),
            pltpu.VMEM((2, 6, 2, HALF, WIDE), bf16),
            pltpu.VMEM((2, 2, 2, HALF, WIDE), bf16),
            pltpu.VMEM((2, 4, HALF, WIDE), bf16),
            pltpu.VMEM((2, 3, HALF, WIDE), bf16),
            pltpu.VMEM((2, HALF, WIDE), f32),
            pltpu.VMEM((WIDE + 16, 128), f32),
            pltpu.VMEM((8, 2, MSG, 128), bf16),
            pltpu.VMEM((2, 8, MSG, 128), bf16),
            pltpu.SemaphoreType.DMA((NBLK,)),
            pltpu.SemaphoreType.DMA((4,)),
            pltpu.SemaphoreType.DMA((4,)),
            pltpu.SemaphoreType.DMA((2, 6)),
            pltpu.SemaphoreType.DMA((2, 6)),
            pltpu.SemaphoreType.DMA((2, 4)),
            pltpu.SemaphoreType.DMA((2, 3)),
            pltpu.SemaphoreType.DMA((8, 2)),
            pltpu.SemaphoreType.DMA((2, 8)),
        ],
        compiler_params=pltpu.CompilerParams(
            collective_id=0, has_side_effects=True, vmem_limit_bytes=56 * 1024 * 1024
        ),
        name="transform",
    )(integrals.reshape(NBLK * DEPTH, VW), jnp.swapaxes(bra_rows, 2, 3), jnp.swapaxes(ket_rows, 2, 3), block_count, pair_count)
    return out.reshape(2, 4, 24, 36)


def solution(mesh):
    split = ("ao", "gen", "act")
    in_specs = (
        P(split, None, None, None),
        P(split, None, None, None),
        P(split, None, None, None),
        P(split),
        P(split),
    )
    out_specs = P(None, "gen", "act", "ao")
    return jax.shard_map(local, mesh=mesh, in_specs=in_specs, out_specs=out_specs, check_vma=False)
```

```python
import jax
import jax.numpy as jnp
from jax import lax
from jax.experimental import pallas as pl
from jax.experimental.pallas import tpu as pltpu
from jax.sharding import PartitionSpec as P

MESH = pl.DeviceIdType.MESH
NBLK = 12
DEPTH = 256
VW = 1152
ROWS = 96
WIDE = 640
MSG = 40


def kernel(ints_hbm, bra_hbm, ket_hbm, block_count, pair_count, out_ref,
           ints, acc, bra_ref, ket_ref, bra_wide, ket_wide, weights, psend, precv, s1, r1, joined, s2, r2, mine, turned, s3, r3,
           small_sem, load_sem, p_send, p_recv, s1_send, s1_recv, s2_send, s2_recv, s3_send, s3_recv):
    ao, gen, act = lax.axis_index("ao"), lax.axis_index("gen"), lax.axis_index("act")
    core = ao % 2
    z = (ao // 2) % 8
    x_lo = ao // 16
    x_hi = act
    x = 2 * x_hi + x_lo
    y = gen

    def device(xx, yy, zz, cc):
        return (((xx % 2) * 8 + zz) * 2 + cc, yy, xx // 2)

    def first(d):
        return device(core * x + (1 - core) * d, core * d + (1 - core) * y, z, core)

    def second(d):
        return device(core * d + (1 - core) * x, core * y + (1 - core) * d, z, core)

    me1 = (1 - core) * x + core * y
    me2 = (1 - core) * y + core * x

    small = [
        pltpu.make_async_copy(bra_hbm, bra_ref, small_sem.at[0]),
        pltpu.make_async_copy(ket_hbm, ket_ref, small_sem.at[1]),
    ]
    for copy in small:
        copy.start()
    loads = []
    for b in range(NBLK):
        rows = pl.ds(b * DEPTH, DEPTH)
        loads.append(pltpu.make_async_copy(ints_hbm.at[rows], ints.at[rows], load_sem.at[b]))
    for copy in loads[: NBLK // 2]:
        copy.start()

    barrier = pltpu.get_barrier_semaphore()
    pl.semaphore_signal(barrier, inc=1, device_id=device(x, y, z, 1 - core), device_id_type=MESH)
    for k in (1, 2, 3):
        pl.semaphore_signal(barrier, inc=1, device_id=first((me1 + k) % 4), device_id_type=MESH)
        pl.semaphore_signal(barrier, inc=1, device_id=second((me2 + k) % 4), device_id_type=MESH)
    for k in range(1, 8):
        for c in (0, 1):
            pl.semaphore_signal(barrier, inc=1, device_id=device(x, y, (z + k) % 8, c), device_id_type=MESH)

    lane = lax.broadcasted_iota(jnp.int32, (48, 128), 1)
    live_blocks = block_count[0]

    def build(b, carry):
        live = jnp.where(b < live_blocks, pair_count[b], 0)
        keep = lane < live
        for r in (0, 1):
            bra_wide[r] = bra_ref[b, r].astype(jnp.float32)
            ket_wide[r] = jnp.where(keep, ket_ref[b, r].astype(jnp.float32), 0.0)
        low = pl.ds(pl.multiple_of(b * DEPTH, DEPTH), 128)
        high = pl.ds(pl.multiple_of(b * DEPTH + 128, 128), 128)
        for xh in (0, 1):
            kr = ket_wide[0, xh * 24 : xh * 24 + 24]
            ki = ket_wide[1, xh * 24 : xh * 24 + 24]
            for yy in range(4):
                re, im = [], []
                for p in range(4):
                    br = bra_wide[0, yy * 4 + p : yy * 4 + p + 1]
                    bi = bra_wide[1, yy * 4 + p : yy * 4 + p + 1]
                    re.append(br * kr + bi * ki)
                    im.append(br * ki - bi * kr)
                re = jnp.concatenate(re, axis=0)
                im = jnp.concatenate(im, axis=0)
                re_low = re.astype(jnp.bfloat16)
                im_low = im.astype(jnp.bfloat16)
                weights[0, xh * 4 + yy, :, low] = re_low
                weights[0, xh * 4 + yy, :, high] = -im_low
                weights[1, yy * 2 + xh, :, low] = im_low
                weights[1, yy * 2 + xh, :, high] = re_low
        return carry

    for copy in small:
        copy.wait()
    lax.fori_loop(0, NBLK // 2, build, 0)
    for copy in loads[NBLK // 2 :]:
        copy.start()
    lax.fori_loop(NBLK // 2, NBLK, build, 0)

    other_x = 1 - x_hi

    def groups(part, t):
        from_x = (other_x if t < 2 else x_hi) * 4 + 2 * (t % 2)
        near, far = (y + 1) % 4, (y + 3) % 4
        pairs = (((y + 2) % 4, 0), ((y + 2) % 4, 1)), ((near, 0), (far, 0)), ((near, 1), (far, 1)), ((y, 0), (y, 1))
        return [(1 - part) * (from_x + j) + part * (pairs[t][j][0] * 2 + pairs[t][j][1]) for j in (0, 1)]

    def product(part, t, depth=slice(None)):
        lhs = jnp.concatenate([weights[part, g, :, depth] for g in groups(part, t)], axis=0)
        return jnp.dot(lhs, ints[depth], preferred_element_type=jnp.float32)

    def p_copy(t):
        return pltpu.make_async_remote_copy(
            src_ref=psend.at[t], dst_ref=precv.at[t], send_sem=p_send.at[t], recv_sem=p_recv.at[t],
            device_id=device(x, y, z, 1 - core), device_id_type=MESH)

    def for_partner(t):
        if t == 0:
            middle = NBLK * DEPTH // 2
            for copy in loads[: NBLK // 2]:
                copy.wait()
            acc[...] = product(1 - core, t, slice(0, middle))
            for copy in loads[NBLK // 2 :]:
                copy.wait()
            psend[t] = (acc[...] + product(1 - core, t, slice(middle, None))).astype(jnp.bfloat16)
            pl.semaphore_wait(barrier, 21)
        else:
            psend[t] = product(1 - core, t).astype(jnp.bfloat16)
        p_copy(t).start()

    right, left = (me1 + 1) % 4, (me1 + 3) % 4
    side = {0: right, 1: left}

    def remote1(src_ref, dst_ref, k, to):
        return pltpu.make_async_remote_copy(
            src_ref=src_ref, dst_ref=dst_ref, send_sem=s1_send.at[k], recv_sem=s1_recv.at[k],
            device_id=first(side[to]), device_id_type=MESH)

    def opposite(to):
        return remote1(s1.at[(me1 + 2) % 4, to], r1.at[to], to, to)

    def plain(to):
        return remote1(s1.at[side[to], 1 - to], r1.at[2 + to], 2 + to, to)

    def relayed(to):
        return remote1(joined.at[to], r1.at[4 + to], 4 + to, to)

    def relay(to):
        opposite(to).wait_recv()
        for j in (0, 1):
            joined[to, j] = (s1[side[to], to, j].astype(jnp.float32) + r1[to, j].astype(jnp.float32)).astype(jnp.bfloat16)
        relayed(to).start()

    def for_self(t):
        p_copy(t).wait_recv()
        value = product(core, t) + precv[t].astype(jnp.float32)
        low = value.astype(jnp.bfloat16)
        from_x = 2 * (other_x if t < 2 else x_hi)
        for j, g in enumerate(groups(core, t)):
            for xl in (0, 1):
                d1 = (1 - core) * (from_x + xl) + core * (g // 2)
                half = (1 - core) * (t % 2) + core * (g % 2)
                spot = (1 - core) * j + core * xl
                s1[d1, half, spot] = low[j * ROWS : (j + 1) * ROWS, xl * 512 : xl * 512 + WIDE]

    is_y = core == 1
    even = jnp.logical_and(core == 0, x_lo == 0)
    odd = jnp.logical_and(core == 0, x_lo == 1)

    def when(*conditions):
        condition = conditions[0]
        for extra in conditions[1:]:
            condition = jnp.logical_or(condition, extra)
        return pl.when(condition)

    for_partner(0)
    for_partner(1)
    for_self(0)
    opposite(0).start()

    @when(is_y)
    def _():
        opposite(1).start()

    @when(even)
    def _():
        plain(1).start()

    for_partner(2)
    for_self(1)

    @when(even, odd)
    def _():
        opposite(1).start()

    @when(is_y)
    def _():
        plain(1).start()

    @when(odd)
    def _():
        plain(0).start()

    for_partner(3)

    @when(is_y, odd)
    def _():
        relay(0)

    for_self(2)

    @when(is_y)
    def _():
        plain(0).start()
        relay(1)

    @when(odd)
    def _():
        plain(1).start()

    @when(even)
    def _():
        relay(0)

    for_self(3)

    @when(even)
    def _():
        plain(0).start()

    @when(even, odd)
    def _():
        relay(1)

    def s2_copy(d2, slot):
        return pltpu.make_async_remote_copy(
            src_ref=s2.at[d2], dst_ref=r2.at[slot], send_sem=s2_send.at[d2], recv_sem=s2_recv.at[slot],
            device_id=second(d2), device_id_type=MESH)

    for half in (0, 1):
        relayed(half).wait_recv()
        plain(1 - half).wait_recv()
        for j in (0, 1):
            d2 = 2 * half + j
            total = s1[me1, half, j].astype(jnp.float32) + r1[4 + half, j].astype(jnp.float32) + r1[3 - half, j].astype(jnp.float32)
            s2[d2] = total.astype(jnp.bfloat16)

            @pl.when(d2 == me2)
            def _():
                mine[...] = total

            @pl.when(d2 != me2)
            def _():
                s2_copy(d2, (me2 - d2 + 7) % 4 % 3).start()

    for slot in range(3):
        s2_copy(0, slot).wait_recv()
    total = mine[...]
    for slot in range(3):
        total = total + r2[slot].astype(jnp.float32)

    pad = jnp.zeros((32, 128), jnp.float32)
    for tile in range(5):
        turned[tile * 128 : (tile + 1) * 128] = jnp.concatenate([total[:, tile * 128 : (tile + 1) * 128], pad], axis=0).T
    turned[WIDE:] = jnp.zeros((16, 128), jnp.float32)

    def s3_copy(k, c):
        zz = (z + k) % 8
        return pltpu.make_async_remote_copy(
            src_ref=s3.at[zz, c], dst_ref=r3.at[core, z], send_sem=s3_send.at[k, c], recv_sem=s3_recv.at[core, z],
            device_id=device(x, y, zz, c), device_id_type=MESH)

    for k in (4, 3, 5, 2, 6, 1, 7, 0):
        zz = (z + k) % 8
        for c in (0, 1):
            start = pl.multiple_of(64 * x_lo + 72 * zz + 32 * c, 8)
            s3[zz, c] = turned[pl.ds(start, MSG)].astype(jnp.bfloat16)
            if k > 0:
                s3_copy(k, c).start()
            else:

                @pl.when(core != c)
                def _():
                    s3_copy(k, c).start()

    r3[core, z] = s3[z, core]
    for k in range(8):
        zz = (z + k) % 8
        for c in (0, 1):

            def arrival():
                return pltpu.make_async_remote_copy(
                    src_ref=s3.at[0, 0], dst_ref=r3.at[c, zz], send_sem=s3_send.at[0, 0], recv_sem=s3_recv.at[c, zz],
                    device_id=device(x, y, z, 1 - core), device_id_type=MESH)

            if k > 0:
                arrival().wait_recv()
            else:

                @pl.when(core != c)
                def _():
                    arrival().wait_recv()

    fill = jnp.zeros((128 - MSG, 128), jnp.float32)
    for r in (0, 1):
        piece = r3[r, 0].astype(jnp.float32)
        for zz in range(1, 8):
            piece = piece + r3[r, zz].astype(jnp.float32)
        back = jnp.concatenate([piece, fill], axis=0).T
        out_ref[r] = jnp.where(core == 0, back[:ROWS, :36], back[:ROWS, 4:40])

    for t in range(4):
        p_copy(t).wait_send()
    for to in (0, 1):
        opposite(to).wait_send()
        plain(to).wait_send()
        relayed(to).wait_send()
    for d2 in range(4):

        @pl.when(d2 != me2)
        def _():
            s2_copy(d2, 0).wait_send()

    for k in range(8):
        for c in (0, 1):
            if k > 0:
                s3_copy(k, c).wait_send()
            else:

                @pl.when(core != c)
                def _():
                    s3_copy(k, c).wait_send()


def local(integrals, bra_rows, ket_rows, block_count, pair_count):
    bf16, f32 = jnp.bfloat16, jnp.float32
    out = pl.pallas_call(
        kernel,
        out_shape=jax.ShapeDtypeStruct((2, ROWS, 36), f32),
        in_specs=[
            pl.BlockSpec(memory_space=pl.ANY),
            pl.BlockSpec(memory_space=pl.ANY),
            pl.BlockSpec(memory_space=pl.ANY),
            pl.BlockSpec(memory_space=pltpu.SMEM),
            pl.BlockSpec(memory_space=pltpu.SMEM),
        ],
        out_specs=pl.BlockSpec(memory_space=pltpu.VMEM),
        scratch_shapes=[
            pltpu.VMEM((NBLK * DEPTH, VW), bf16),
            pltpu.VMEM((2 * ROWS, VW), f32),
            pltpu.VMEM((NBLK, 2, 16, 128), bf16),
            pltpu.VMEM((NBLK, 2, 48, 128), bf16),
            pltpu.VMEM((2, 16, 128), f32),
            pltpu.VMEM((2, 48, 128), f32),
            pltpu.VMEM((2, 8, ROWS, NBLK * DEPTH), bf16),
            pltpu.VMEM((4, 2 * ROWS, VW), bf16),
            pltpu.VMEM((4, 2 * ROWS, VW), bf16),
            pltpu.VMEM((4, 2, 2, ROWS, WIDE), bf16),
            pltpu.VMEM((6, 2, ROWS, WIDE), bf16),
            pltpu.VMEM((2, 2, ROWS, WIDE), bf16),
            pltpu.VMEM((4, ROWS, WIDE), bf16),
            pltpu.VMEM((3, ROWS, WIDE), bf16),
            pltpu.VMEM((ROWS, WIDE), f32),
            pltpu.VMEM((WIDE + 16, 128), f32),
            pltpu.VMEM((8, 2, MSG, 128), bf16),
            pltpu.VMEM((2, 8, MSG, 128), bf16),
            pltpu.SemaphoreType.DMA((2,)),
            pltpu.SemaphoreType.DMA((NBLK,)),
            pltpu.SemaphoreType.DMA((4,)),
            pltpu.SemaphoreType.DMA((4,)),
            pltpu.SemaphoreType.DMA((6,)),
            pltpu.SemaphoreType.DMA((6,)),
            pltpu.SemaphoreType.DMA((4,)),
            pltpu.SemaphoreType.DMA((3,)),
            pltpu.SemaphoreType.DMA((8, 2)),
            pltpu.SemaphoreType.DMA((2, 8)),
        ],
        compiler_params=pltpu.CompilerParams(
            collective_id=0, has_side_effects=True, vmem_limit_bytes=63 * 1024 * 1024
        ),
        name="transform",
    )(integrals.reshape(NBLK * DEPTH, VW), jnp.swapaxes(bra_rows, 2, 3), jnp.swapaxes(ket_rows, 2, 3), block_count, pair_count)
    return out.reshape(2, 4, 24, 36)


def solution(mesh):
    split = ("ao", "gen", "act")
    in_specs = (
        P(split, None, None, None),
        P(split, None, None, None),
        P(split, None, None, None),
        P(split),
        P(split),
    )
    out_specs = P(None, "gen", "act", "ao")
    return jax.shard_map(local, mesh=mesh, in_specs=in_specs, out_specs=out_specs, check_vma=False)
```
